8 devices in a mesh: rep: 1 (over z), dp: 8 (over x, y, core).
Axes of the slice: x: 2, y: 2, z: 1, core: 2. Of those that a mesh axis runs over, the one named last changes fastest.
Arguments:
- g_w_gate: bfloat16 [8, 2, 1152, 4608], P(('rep', 'dp'))
- g_w_up: bfloat16 [8, 2, 1152, 4608], P(('rep', 'dp'))
- g_w_down: bfloat16 [8, 2, 4608, 1152], P(('rep', 'dp'))
- w_gate: bfloat16 [2, 1152, 4608], replicated
- w_up: bfloat16 [2, 1152, 4608], replicated
- w_down: bfloat16 [2, 4608, 1152], replicated
- m_w_gate: float32 [2, 1152, 4608], P(None, 'dp')
- m_w_up: float32 [2, 1152, 4608], P(None, 'dp')
- m_w_down: float32 [2, 4608, 1152], P(None, 'dp')
- v_w_gate: float32 [2, 1152, 4608], P(None, 'dp')
- v_w_up: float32 [2, 1152, 4608], P(None, 'dp')
- v_w_down: float32 [2, 4608, 1152], P(None, 'dp')
Outputs:
- output 1: bfloat16 [2, 1152, 4608], P('rep')
- output 2: bfloat16 [2, 1152, 4608], P('rep')
- output 3: bfloat16 [2, 4608, 1152], P('rep')
- output 4: float32 [2, 1152, 4608], P('rep', 'dp')
- output 5: float32 [2, 1152, 4608], P('rep', 'dp')
- output 6: float32 [2, 4608, 1152], P('rep', 'dp')
- output 7: float32 [2, 1152, 4608], P('rep', 'dp')
- output 8: float32 [2, 1152, 4608], P('rep', 'dp')
- output 9: float32 [2, 4608, 1152], P('rep', 'dp')
All inputs are finite; a program needn't handle non-finite values.
Results may differ from the reference program's by a relative error of at most 0.022.
Values are sent between devices in bfloat16 or wider.
A program may use at most 2 GiB of HBM per device.

```python
import jax
import jax.numpy as jnp
from jax import lax

DEVICES = 8
D = 1152
FF = 4608
LAYERS = 2
NAMES = ("w_gate", "w_up", "w_down")
SHAPES = {"w_gate": (LAYERS, D, FF), "w_up": (LAYERS, D, FF), "w_down": (LAYERS, FF, D)}


def setup_inputs(seed: int = 0, part: int = 0) -> dict:
    kz, *keys = jax.random.split(jax.random.key(seed), 1 + 5 * len(NAMES))
    loud = 2.0 ** jax.random.uniform(kz, (), jnp.float32, -1.0, 1.0)
    drawn = {}
    for name, key, both in zip(NAMES, keys[:3], keys[3:6], strict=True):
        own = jax.random.normal(jax.random.fold_in(key, part), (DEVICES, *SHAPES[name]), jnp.float32)
        shared = jax.random.normal(jax.random.fold_in(both, part), SHAPES[name], jnp.float32)
        drawn["g_" + name] = (loud * (0.7 * shared / DEVICES + 0.7 * own * DEVICES**-0.5)).astype(jnp.bfloat16)
    for name, key in zip(NAMES, keys[6:9], strict=True):
        drawn[name] = (jax.random.normal(key, SHAPES[name], jnp.float32) * SHAPES[name][1] ** -0.5).astype(jnp.bfloat16)
    for name, key in zip(NAMES, keys[9:12], strict=True):
        drawn["m_" + name] = loud * 0.5 * jax.random.normal(key, SHAPES[name], jnp.float32)
    for name, key in zip(NAMES, keys[12:15], strict=True):
        drawn["v_" + name] = loud * loud * jax.random.uniform(key, SHAPES[name], jnp.float32, 0.5, 1.5)
    return drawn


def adamw(w, m, v, g):
    m = 0.9 * m + 0.1 * g
    v = 0.95 * v + 0.05 * g * g
    step = m * lax.rsqrt(v + 1e-8) + 0.1 * w
    return (w - 0.02 * step).astype(jnp.bfloat16), m, v


def clipped(gradients, sum_of_squares, count):
    factor = jnp.minimum(1.0, 0.5 * lax.rsqrt(sum_of_squares / count + 1e-30))
    return [g * factor for g in gradients]


def reference(g_w_gate, g_w_up, g_w_down, w_gate, w_up, w_down, m_w_gate, m_w_up, m_w_down, v_w_gate, v_w_up, v_w_down):
    def total(terms):
        return lax.scan(lambda so_far, term: (so_far + term.astype(jnp.float32), None), jnp.zeros(terms.shape[1:], jnp.float32), terms)[0]

    gradients = [total(terms).astype(jnp.bfloat16).astype(jnp.float32) for terms in (g_w_gate, g_w_up, g_w_down)]
    gradients = clipped(gradients, sum(jnp.sum(g * g) for g in gradients), sum(g.size for g in gradients))
    new = [
        adamw(w.astype(jnp.float32), m, v, g)
        for w, m, v, g in zip((w_gate, w_up, w_down), (m_w_gate, m_w_up, m_w_down), (v_w_gate, v_w_up, v_w_down), gradients, strict=True)
    ]
    return tuple(one[which] for which in range(3) for one in new)
```

```python
import jax
import jax.numpy as jnp
from jax import lax
from jax.experimental import pallas as pl
from jax.experimental.pallas import tpu as pltpu
from jax.sharding import PartitionSpec as P

MESH = pl.DeviceIdType.MESH
F32, BF16 = jnp.float32, jnp.bfloat16
LAYERS, D, FF = 2, 1152, 4608
R, C, Q = 144, 1152, 4
CHUNKS = 3 * Q
STEP = 16
COUNT = LAYERS * 3 * D * FF


def chunk(ref, j, layer, d, lead=()):
    w, q = divmod(j, Q)
    if w < 2:
        return ref[w].at[*lead, layer, pl.ds(pl.multiple_of(d * R, R), R), pl.ds(q * C, C)]
    return ref[w].at[*lead, layer, pl.ds(pl.multiple_of(d * (Q * R) + q * R, R), R), :]


def own_chunk(ref, j, layer):
    w, q = divmod(j, Q)
    if w < 2:
        return ref[w].at[layer, :, pl.ds(q * C, C)]
    return ref[w].at[layer, pl.ds(q * R, R), :]


def neighbours():
    me = lax.axis_index("dp")
    x = lax.rem(me + 4, 8)
    y = me + 2 - 4 * lax.rem(me // 2, 2)
    xy = lax.rem(y + 4, 8)
    other = me + 1 - 2 * lax.rem(me, 2)
    return me, x, y, xy, other


def remote(src, dst, send, recv, to):
    return pltpu.make_async_remote_copy(src_ref=src, dst_ref=dst, send_sem=send, recv_sem=recv, device_id={"dp": to}, device_id_type=MESH)


def enter(peers):
    barrier = pltpu.get_barrier_semaphore()
    for p in peers:
        pl.semaphore_signal(barrier, inc=1, device_id={"dp": p}, device_id_type=MESH)
    pl.semaphore_wait(barrier, len(peers))


def scatter_kernel(*refs):
    g, (g_out, ss_out, landed) = refs[:3], refs[3:6]
    lo, lp, s1, s2, r1, r2, stage, acc, mine, every = refs[6:16]
    d_send, d_recv, l_sem, s1_send, r1_recv, s2_send, r2_recv, o_sem, e_send, e_recv = refs[16:]
    me, x, y, xy, other = neighbours()
    my_c = lax.rem(me, 2)
    enter([lax.rem(me + k, 8) for k in range(1, 8)])

    blocks = [me, x, y, xy]
    flip = 1 - 2 * my_c
    first = [(0, 3), (1, 3), (0, 1), (1, 2)]
    second = [(0, 2), (1, 1)]
    last = [(0, 0), (1, 0)]
    everything = first + second + last

    def swap(j, i):
        layer, k = everything[i]
        return remote(chunk(g, j, layer, blocks[k] + flip, (0,)), landed.at[j, i], d_send.at[j, i], d_recv.at[j, i], other)

    for j in range(CHUNKS):
        for i in range(8):
            swap(j, i).start()

    groups = [range(0, 4), range(4, 6), range(6, 8)]

    def loads(j, group):
        slot = j % 2
        out = []
        for i in groups[group]:
            layer, k = everything[i]
            out.append(pltpu.make_async_copy(chunk(g, j, layer, blocks[k], (0,)), lo.at[slot, i], l_sem.at[slot, i, 0]))
            out.append(pltpu.make_async_copy(landed.at[j, i], lp.at[slot, i], l_sem.at[slot, i, 1]))
        return out

    def start_loads(j, group):
        for i in groups[group]:
            swap(j, i).wait_recv()
        for c in loads(j, group):
            c.start()

    def wait_loads(j, group):
        for c in loads(j, group):
            c.wait()

    def add(dst, *terms):
        @pl.loop(0, R // STEP)
        def _(s):
            rows = pl.ds(pl.multiple_of(s * STEP, STEP), STEP)
            total = terms[0][rows, :].astype(F32)
            for t in terms[1:]:
                total = total + t[rows, :].astype(F32)
            dst[rows, :] = total.astype(BF16)

    def first_hop(j, n):
        to = (x, y, x, y)[n]
        at = (1, 3, 0, 2)[n]
        return remote(s1.at[j % 3, n], r1.at[j, at], s1_send.at[j, n], r1_recv.at[j, at], to)

    def second_hop(j, n):
        to = (y, x)[n]
        return remote(s2.at[j % 3, n], r2.at[j, n], s2_send.at[j, n], r2_recv.at[j, n], to)

    def arrived(j, at):
        n = (2, 0, 3, 1)[at]
        first_hop(j, n).wait_recv()

    def out(j, n):
        return pltpu.make_async_copy(stage.at[j % 2, n], g_out.at[n, j], o_sem.at[j % 2, n])

    acc[...] = jnp.zeros_like(acc)
    start_loads(0, 0)
    for t in range(CHUNKS + 2):
        j = t
        if j < CHUNKS:
            wait_loads(j, 0)
            if j >= 3:
                for n in range(4):
                    first_hop(j - 3, n).wait_send()
            for n in range(4):
                add(s1.at[j % 3, n], lo.at[j % 2, n], lp.at[j % 2, n])
                first_hop(j, n).start()
            if j + 1 < CHUNKS:
                start_loads(j + 1, 0)
            start_loads(j, 1)
        j = t - 1
        if 0 <= j < CHUNKS:
            wait_loads(j, 1)
            if j >= 3:
                for n in range(2):
                    second_hop(j - 3, n).wait_send()
            for n, at in ((0, 1), (1, 3)):
                arrived(j, at)
                add(s2.at[j % 3, n], lo.at[j % 2, 4 + n], lp.at[j % 2, 4 + n], r1.at[j, at])
                second_hop(j, n).start()
            start_loads(j, 2)
        j = t - 2
        if 0 <= j < CHUNKS:
            wait_loads(j, 2)
            for n, at in ((0, 0), (1, 2)):
                arrived(j, at)
                second_hop(j, n).wait_recv()
                if j >= 2:
                    out(j - 2, n).wait()
                a, b, c, e, dst = lo.at[j % 2, 6 + n], lp.at[j % 2, 6 + n], r1.at[j, at], r2.at[j, n], stage.at[j % 2, n]

                @pl.loop(0, R // STEP)
                def _(s):
                    rows = pl.ds(pl.multiple_of(s * STEP, STEP), STEP)
                    total = (a[rows, :].astype(F32) + b[rows, :].astype(F32)) + c[rows, :].astype(F32) + e[rows, :].astype(F32)
                    total = total.astype(BF16)
                    dst[rows, :] = total
                    total = total.astype(F32)
                    squares = total * total
                    acc[...] += squares[:8] + squares[8:]

                out(j, n).start()

    tile = acc[:, :128]
    for i in range(1, C // 128):
        tile = tile + acc[:, i * 128 : (i + 1) * 128]
    mine[...] = tile
    every[me] = tile
    def tell(k):
        return remote(mine, every.at[me], e_send.at[k], e_recv.at[k], lax.rem(me + k, 8))

    def told(k):
        return remote(mine, every.at[lax.rem(me + 8 - k, 8)], e_send.at[k], e_recv.at[k], lax.rem(me + k, 8))

    for k in range(1, 8):
        tell(k).start()
    for k in range(1, 8):
        told(k).wait_recv()
    total = every[0]
    for k in range(1, 8):
        total = total + every[k]
    ss_out[...] = jnp.broadcast_to(jnp.sum(total, keepdims=True), (8, 128))
    for k in range(1, 8):
        tell(k).wait_send()
    for j in range(CHUNKS):
        for i in range(8):
            swap(j, i).wait_send()
    for j in range(CHUNKS - 3, CHUNKS):
        for n in range(4):
            first_hop(j, n).wait_send()
        for n in range(2):
            second_hop(j, n).wait_send()
    for j in range(CHUNKS - 2, CHUNKS):
        for n in range(2):
            out(j, n).wait()


def scatter(terms):
    any_ = pl.BlockSpec(memory_space=pl.ANY)
    dma = pltpu.SemaphoreType.DMA
    buf = lambda *lead: pltpu.VMEM((*lead, R, C), BF16)
    return pl.pallas_call(
        scatter_kernel,
        name="scatter_sum",
        out_shape=[
            jax.ShapeDtypeStruct((2, CHUNKS, R, C), BF16),
            jax.ShapeDtypeStruct((8, 128), F32),
            jax.ShapeDtypeStruct((CHUNKS, 8, R, C), BF16),
        ],
        in_specs=[any_] * 3,
        out_specs=[any_, pl.BlockSpec(memory_space=pltpu.VMEM), any_],
        scratch_shapes=[
            buf(2, 8), buf(2, 8), buf(3, 4), buf(3, 2), buf(CHUNKS, 4), buf(CHUNKS, 2), buf(2, 2),
            pltpu.VMEM((8, C), F32), pltpu.VMEM((8, 128), F32), pltpu.VMEM((8, 8, 128), F32),
            dma((CHUNKS, 8)), dma((CHUNKS, 8)), dma((2, 8, 2)), dma((CHUNKS, 4)), dma((CHUNKS, 4)),
            dma((CHUNKS, 2)), dma((CHUNKS, 2)), dma((2, 2)), dma((8,)), dma((8,)),
        ],
        compiler_params=pltpu.CompilerParams(collective_id=0, has_side_effects=True, vmem_limit_bytes=52 * 2**20),
    )(*terms)


def adamw_kernel(me_ref, ss, g_ref, w_ref, m_ref, v_ref, new_w, new_m, new_v):
    factor = jnp.minimum(1.0, 0.5 * lax.rsqrt(ss[...] / COUNT + 1e-30))[:1, :1]

    @pl.loop(0, R // STEP)
    def _(s):
        rows = pl.ds(pl.multiple_of(s * STEP, STEP), STEP)
        g = g_ref[0, 0, rows, :].astype(F32) * factor
        w = w_ref[0, rows, :].astype(F32)
        m = 0.9 * m_ref[0, rows, :] + 0.1 * g
        v = 0.95 * v_ref[0, rows, :] + 0.05 * g * g
        step = m * lax.rsqrt(v + 1e-8) + 0.1 * w
        new_w[0, rows, :] = (w - 0.02 * step).astype(BF16)
        new_m[0, rows, :] = m
        new_v[0, rows, :] = v


def adamw(me, ss, g, which, w, m, v):
    wide = which < 2
    own = pl.BlockSpec((1, R, C), (lambda l, q, me: (l, 0, q)) if wide else (lambda l, q, me: (l, q, 0)))
    whole = pl.BlockSpec((1, R, C), (lambda l, q, me: (l, me[0], q)) if wide else (lambda l, q, me: (l, me[0] * Q + q, 0)))
    return pl.pallas_call(
        adamw_kernel,
        name=f"adamw_{which}",
        out_shape=[jax.ShapeDtypeStruct(m.shape, BF16), jax.ShapeDtypeStruct(m.shape, F32), jax.ShapeDtypeStruct(m.shape, F32)],
        grid_spec=pltpu.PrefetchScalarGridSpec(
            num_scalar_prefetch=1,
            grid=(LAYERS, Q),
            in_specs=[
                pl.BlockSpec((8, 128), lambda l, q, me: (0, 0)),
                pl.BlockSpec((1, 1, R, C), lambda l, q, me: (l, which * Q + q, 0, 0)),
                whole, own, own,
            ],
            out_specs=[own, own, own],
        ),
        compiler_params=pltpu.CompilerParams(vmem_limit_bytes=24 * 2**20),
    )(me, ss, g, w, m, v)


def gather_kernel(*refs):
    new, whole = refs[:3], refs[3:6]
    own, l_sem, o_sem, send, recv, d_send, d_recv = refs[6:]
    me, x, y, xy, other = neighbours()
    flip = 1 - 2 * lax.rem(me, 2)
    enter([x, y, other])
    blocks = [me, x, y, xy]
    every = [(layer, j) for j in range(CHUNKS) for layer in range(2)]

    def load(layer, j):
        return pltpu.make_async_copy(own_chunk(new, j, layer), own.at[layer, j], l_sem.at[layer, j])

    def store(layer, j):
        return pltpu.make_async_copy(own.at[layer, j], chunk(whole, j, layer, me), o_sem.at[layer, j])

    def hop(layer, j, h):
        if h < 2:
            src, d, to = own.at[layer, j], me, (x, y)[h]
        else:
            d = (y, x)[layer]
            src, to = chunk(whole, j, layer, d), (x, y)[layer]
        return remote(src, chunk(whole, j, layer, d), send.at[layer, j, h], recv.at[layer, j, h], to)

    def came(layer, j, h):
        d = (x, y)[h] if h < 2 else xy
        dst = chunk(whole, j, layer, d)
        return remote(dst, dst, send.at[layer, j, h], recv.at[layer, j, h], x)

    def share(layer, j, k):
        d = blocks[k]
        src = own.at[layer, j] if k == 0 else chunk(whole, j, layer, d)
        return remote(src, chunk(whole, j, layer, d), d_send.at[layer, j, k], d_recv.at[layer, j, k], other)

    def shared(layer, j, k):
        dst = chunk(whole, j, layer, blocks[k] + flip)
        return remote(dst, dst, d_send.at[layer, j, k], d_recv.at[layer, j, k], other)

    for layer, j in every:
        load(layer, j).start()
    for layer, j in every:
        load(layer, j).wait()
        hop(layer, j, 1 - layer).start()
    for layer, j in every:
        hop(layer, j, layer).start()
        share(layer, j, 0).start()
        store(layer, j).start()
    for layer, j in every:
        h = 1 - layer
        came(layer, j, h).wait_recv()
        hop(layer, j, 2).start()
        share(layer, j, 1 + h).start()
    for layer, j in every:
        came(layer, j, layer).wait_recv()
        share(layer, j, 1 + layer).start()
    for layer, j in every:
        came(layer, j, 2).wait_recv()
        share(layer, j, 3).start()
    for layer, j in every:
        store(layer, j).wait()
        for h in range(3):
            hop(layer, j, h).wait_send()
        for k in range(4):
            share(layer, j, k).wait_send()
            shared(layer, j, k).wait_recv()


def gather(new, like):
    any_ = pl.BlockSpec(memory_space=pl.ANY)
    dma = pltpu.SemaphoreType.DMA
    return pl.pallas_call(
        gather_kernel,
        name="gather",
        out_shape=[jax.ShapeDtypeStruct(w.shape, BF16) for w in like],
        in_specs=[any_] * 3,
        out_specs=[any_] * 3,
        scratch_shapes=[
            pltpu.VMEM((2, CHUNKS, R, C), BF16),
            dma((2, CHUNKS)), dma((2, CHUNKS)), dma((2, CHUNKS, 3)), dma((2, CHUNKS, 3)),
            dma((2, CHUNKS, 4)), dma((2, CHUNKS, 4)),
        ],
        compiler_params=pltpu.CompilerParams(collective_id=1, has_side_effects=True, vmem_limit_bytes=12 * 2**20),
    )(*new)


def solution(mesh):
    def step(*arrays):
        terms, weights, m, v = (arrays[i : i + 3] for i in (0, 3, 6, 9))
        g, squares, _ = scatter(terms)
        me = lax.axis_index("dp").astype(jnp.int32).reshape(1)
        new = [adamw(me, squares, g, i, weights[i], m[i], v[i]) for i in range(3)]
        whole = gather([one[0] for one in new], weights)
        return (*whole, *(one[1] for one in new), *(one[2] for one in new))

    all_of, cut = P(None, None, None), P(None, "dp", None)
    return jax.shard_map(
        step,
        mesh=mesh,
        in_specs=(P(("rep", "dp"), None, None, None),) * 3 + (all_of,) * 3 + (cut,) * 6,
        out_specs=(P("rep", None, None),) * 3 + (P("rep", "dp", None),) * 6,
        check_vma=False,
    )
```

```python
import jax
import jax.numpy as jnp
from jax import lax
from jax.experimental import pallas as pl
from jax.experimental.pallas import tpu as pltpu
from jax.sharding import PartitionSpec as P

MESH = pl.DeviceIdType.MESH
F32, BF16 = jnp.float32, jnp.bfloat16
LAYERS, D, FF = 2, 1152, 4608
R, C, Q = 144, 1152, 4
CHUNKS = 3 * Q
KEPT = 6
STEP = 16
COUNT = LAYERS * 3 * D * FF
AHEAD = 4
SLOTS = 24
COST = pl.CostEstimate(flops=10**10, bytes_accessed=3 * 10**7, transcendentals=0)


def chunk(ref, j, layer, d, lead=()):
    w, q = divmod(j, Q)
    if w < 2:
        return ref[w].at[*lead, layer, pl.ds(pl.multiple_of(d * R, R), R), pl.ds(q * C, C)]
    return ref[w].at[*lead, layer, pl.ds(pl.multiple_of(d * (Q * R) + q * R, R), R), :]


def own_chunk(ref, j, layer):
    w, q = divmod(j, Q)
    if w < 2:
        return ref[w].at[layer, :, pl.ds(q * C, C)]
    return ref[w].at[layer, pl.ds(q * R, R), :]


def clip_factor(squares):
    return jnp.minimum(1.0, 0.5 * lax.rsqrt(squares / COUNT + 1e-30))


def row_loop(body):
    @pl.loop(0, R // STEP)
    def _(s):
        body(pl.ds(pl.multiple_of(s * STEP, STEP), STEP))


def neighbours():
    me = lax.axis_index("dp")
    x = lax.rem(me + 4, 8)
    y = me + 2 - 4 * lax.rem(me // 2, 2)
    xy = lax.rem(y + 4, 8)
    other = me + 1 - 2 * lax.rem(me, 2)
    return me, x, y, xy, other


def remote(src, dst, send, recv, to):
    return pltpu.make_async_remote_copy(src_ref=src, dst_ref=dst, send_sem=send, recv_sem=recv, device_id={"dp": to}, device_id_type=MESH)


def enter(peers):
    barrier = pltpu.get_barrier_semaphore()
    for p in peers:
        pl.semaphore_signal(barrier, inc=1, device_id={"dp": p}, device_id_type=MESH)
    pl.semaphore_wait(barrier, len(peers))


def step_kernel(*refs):
    g, w, m, v, refs = refs[:3], refs[3:6], refs[6:9], refs[9:12], refs[12:]
    g_out, ss_out, landed, same, across, later_x, later_y = refs[:7]
    lo, lp, s1, s2, r1, r2, own, m_buf, v_buf, w_buf, acc, mine, every = refs[7:20]
    d_send, d_recv, l_sem, s1_send, r1_recv, s2_send, r2_recv, o_sem, e_send, e_recv = refs[20:30]
    a_sem, t_sem, h_send, h_recv, c_send, c_recv = refs[30:]
    me, x, y, xy, other = neighbours()
    my_c = lax.rem(me, 2)
    enter([lax.rem(me + k, 8) for k in range(1, 8)])

    blocks = [me, x, y, xy]
    flip = 1 - 2 * my_c
    first = [(0, 3), (1, 3), (0, 1), (1, 2)]
    second = [(0, 2), (1, 1)]
    last = [(0, 0), (1, 0)]
    everything = first + second + last

    def swap(j, i):
        layer, k = everything[i]
        to = lp.at[0, i] if j == 0 and i < 4 else landed.at[j, i]
        return remote(chunk(g, j, layer, blocks[k] + flip, (0,)), to, d_send.at[j, i], d_recv.at[j, i], other)

    for j in range(CHUNKS):
        for i in range(8):
            swap(j, i).start()

    groups = [range(0, 4), range(4, 6), range(6, 8)]

    def loads(j, group):
        slot = j % 2
        out = []
        for i in groups[group]:
            layer, k = everything[i]
            out.append(pltpu.make_async_copy(chunk(g, j, layer, blocks[k], (0,)), lo.at[slot, i], l_sem.at[slot, i, 0]))
            if j > 0 or i >= 4:
                out.append(pltpu.make_async_copy(landed.at[j, i], lp.at[slot, i], l_sem.at[slot, i, 1]))
        return out

    def start_loads(j, group):
        for i in groups[group]:
            if j > 0 or i >= 4:
                swap(j, i).wait_recv()
        for c in loads(j, group):
            c.start()

    def wait_loads(j, group):
        for c in loads(j, group):
            c.wait()

    def add(dst, *terms):
        @pl.loop(0, R // STEP)
        def _(s):
            rows = pl.ds(pl.multiple_of(s * STEP, STEP), STEP)
            total = terms[0][rows, :].astype(F32)
            for t in terms[1:]:
                total = total + t[rows, :].astype(F32)
            dst[rows, :] = total.astype(BF16)

    def first_hop(j, n):
        to = (x, y, x, y)[n]
        at = (1, 3, 0, 2)[n]
        return remote(s1.at[j % 3, n], r1.at[j, at], s1_send.at[j, n], r1_recv.at[j, at], to)

    def second_hop(j, n):
        to = (y, x)[n]
        return remote(s2.at[j % 3, n], r2.at[j, n], s2_send.at[j, n], r2_recv.at[j, n], to)

    def arrived(j, at):
        n = (2, 0, 3, 1)[at]
        first_hop(j, n).wait_recv()

    def out(j, n):
        return pltpu.make_async_copy(own.at[n, j], g_out.at[n, j], o_sem.at[n, j])

    items = [(layer, j) for j in range(CHUNKS) for layer in range(2)]

    def state(n):
        layer, j = items[n]
        slot = n % AHEAD
        return [
            pltpu.make_async_copy(own_chunk(m, j, layer), m_buf.at[slot], a_sem.at[slot, 0]),
            pltpu.make_async_copy(own_chunk(v, j, layer), v_buf.at[slot], a_sem.at[slot, 1]),
            pltpu.make_async_copy(chunk(w, j, layer, me), w_buf.at[slot], a_sem.at[slot, 2]),
        ]

    for n in range(AHEAD):
        for c in state(n):
            c.start()

    acc[...] = jnp.zeros_like(acc)
    start_loads(0, 0)
    for t in range(CHUNKS + 2):
        j = t
        if j < CHUNKS:
            wait_loads(j, 0)
            if j >= 3:
                for n in range(4):
                    first_hop(j - 3, n).wait_send()
            for n in range(4):
                if j == 0:
                    swap(j, n).wait_recv()
                add(s1.at[j % 3, n], lo.at[j % 2, n], lp.at[j % 2, n])
                first_hop(j, n).start()
            if j + 1 < CHUNKS:
                start_loads(j + 1, 0)
            start_loads(j, 1)
        j = t - 1
        if 0 <= j < CHUNKS:
            wait_loads(j, 1)
            if j >= 3:
                for n in range(2):
                    second_hop(j - 3, n).wait_send()
            for n, at in ((0, 1), (1, 3)):
                arrived(j, at)
                add(s2.at[j % 3, n], lo.at[j % 2, 4 + n], lp.at[j % 2, 4 + n], r1.at[j, at])
                second_hop(j, n).start()
            start_loads(j, 2)
        j = t - 2
        if 0 <= j < CHUNKS:
            wait_loads(j, 2)
            for n, at in ((0, 0), (1, 2)):
                arrived(j, at)
                second_hop(j, n).wait_recv()
                a, b, c, e, dst = lo.at[j % 2, 6 + n], lp.at[j % 2, 6 + n], r1.at[j, at], r2.at[j, n], own.at[n, j]

                @pl.loop(0, R // STEP)
                def _(s):
                    rows = pl.ds(pl.multiple_of(s * STEP, STEP), STEP)
                    total = (a[rows, :].astype(F32) + b[rows, :].astype(F32)) + c[rows, :].astype(F32) + e[rows, :].astype(F32)
                    total = total.astype(BF16)
                    dst[rows, :] = total
                    total = total.astype(F32)
                    squares = total * total
                    acc[...] += squares[:8] + squares[8:]

                out(j, n).start()

    tile = acc[:, :128]
    for i in range(1, C // 128):
        tile = tile + acc[:, i * 128 : (i + 1) * 128]
    mine[...] = tile
    every[me] = tile
    def tell(k):
        return remote(mine, every.at[me], e_send.at[k], e_recv.at[k], lax.rem(me + k, 8))

    def told(k):
        return remote(mine, every.at[lax.rem(me + 8 - k, 8)], e_send.at[k], e_recv.at[k], lax.rem(me + k, 8))

    for k in range(1, 8):
        tell(k).start()
    for j in range(CHUNKS):
        for n in range(2):
            out(j, n).wait()
    for k in range(1, 8):
        told(k).wait_recv()
    total = every[0]
    for k in range(1, 8):
        total = total + every[k]
    total = jnp.broadcast_to(jnp.sum(total, keepdims=True), (8, 128))
    ss_out[...] = total
    factor = clip_factor(total)[:1, :1]

    def place(k, layer, j):
        if j >= KEPT and (k, layer) == (2, 0):
            return later_x.at[j - KEPT]
        if j >= KEPT and (k, layer) == (1, 1):
            return later_y.at[j - KEPT]
        return same.at[k, layer, j]

    def hop(layer, j, h):
        if h < 2:
            src, k, to = own.at[layer, j], h + 1, (x, y)[h]
        else:
            src, k, to = place(2 - layer, layer, j), 3, (x, y)[layer]
        return remote(src, place(k, layer, j), h_send.at[layer, j, h], h_recv.at[layer, j, h], to)

    def share(layer, j, k):
        src = own.at[layer, j] if k == 0 else place(k, layer, j)
        return remote(src, across.at[k, layer, j], c_send.at[layer, j, k], c_recv.at[layer, j, k], other)

    def keep(layer, j):
        return pltpu.make_async_copy(own.at[layer, j], same.at[0, layer, j], t_sem.at[layer, j])

    for n, (layer, j) in enumerate(items):
        for c in state(n):
            c.wait()
        new, old_w, old_m, old_v = own.at[layer, j], w_buf.at[n % AHEAD], m_buf.at[n % AHEAD], v_buf.at[n % AHEAD]

        def update(rows):
            g = new[rows, :].astype(F32) * factor
            w = old_w[rows, :].astype(F32)
            m = 0.9 * old_m[rows, :] + 0.1 * g
            v = 0.95 * old_v[rows, :] + 0.05 * g * g
            step = m * lax.rsqrt(v + 1e-8) + 0.1 * w
            new[rows, :] = (w - 0.02 * step).astype(BF16)

        row_loop(update)
        hop(layer, j, 1 - layer).start()
        share(layer, j, 0).start()
        keep(layer, j).start()
        if n + AHEAD < len(items):
            for c in state(n + AHEAD):
                c.start()
    for layer, j in items:
        hop(layer, j, layer).start()
    for layer, j in items:
        hop(layer, j, 1 - layer).wait_recv()
        if j < KEPT:
            hop(layer, j, 2).start()
        share(layer, j, 2 - layer).start()
    for layer, j in items:
        hop(layer, j, layer).wait_recv()
        share(layer, j, 1 + layer).start()
    for layer, j in items:
        if j < KEPT:
            hop(layer, j, 2).wait_recv()
            share(layer, j, 3).start()
    for layer, j in items:
        keep(layer, j).wait()
        for h in range(3):
            if h < 2 or j < KEPT:
                hop(layer, j, h).wait_send()
        for k in range(4):
            if k < 3 or j < KEPT:
                share(layer, j, k).wait_send()
                share(layer, j, k).wait_recv()
    for k in range(1, 8):
        tell(k).wait_send()
    for j in range(CHUNKS):
        for i in range(8):
            swap(j, i).wait_send()
    for j in range(CHUNKS - 3, CHUNKS):
        for n in range(4):
            first_hop(j, n).wait_send()
        for n in range(2):
            second_hop(j, n).wait_send()


def step_call(*arrays):
    any_ = pl.BlockSpec(memory_space=pl.ANY)
    dma = pltpu.SemaphoreType.DMA
    buf = lambda *lead: pltpu.VMEM((*lead, R, C), BF16)
    hbm = lambda *lead: jax.ShapeDtypeStruct((*lead, R, C), BF16)
    return pl.pallas_call(
        step_kernel,
        name="scatter_step_gather",
        out_shape=[
            hbm(2, CHUNKS), jax.ShapeDtypeStruct((8, 128), F32), hbm(CHUNKS, 8),
            hbm(4, 2, CHUNKS), hbm(4, 2, CHUNKS), hbm(CHUNKS - KEPT), hbm(CHUNKS - KEPT),
        ],
        in_specs=[any_] * 12,
        out_specs=[any_, pl.BlockSpec(memory_space=pltpu.VMEM)] + [any_] * 5,
        scratch_shapes=[
            buf(2, 8), buf(2, 8), buf(3, 4), buf(3, 2), buf(CHUNKS, 4), buf(CHUNKS, 2), buf(2, CHUNKS),
            pltpu.VMEM((AHEAD, R, C), F32), pltpu.VMEM((AHEAD, R, C), F32), buf(AHEAD),
            pltpu.VMEM((8, C), F32), pltpu.VMEM((8, 128), F32), pltpu.VMEM((8, 8, 128), F32),
            dma((CHUNKS, 8)), dma((CHUNKS, 8)), dma((2, 8, 2)), dma((CHUNKS, 4)), dma((CHUNKS, 4)),
            dma((CHUNKS, 2)), dma((CHUNKS, 2)), dma((2, CHUNKS)), dma((8,)), dma((8,)),
            dma((AHEAD, 3)), dma((2, CHUNKS)), dma((2, CHUNKS, 3)), dma((2, CHUNKS, 3)),
            dma((2, CHUNKS, 4)), dma((2, CHUNKS, 4)),
        ],
        compiler_params=pltpu.CompilerParams(collective_id=0, has_side_effects=True, vmem_limit_bytes=58 * 2**20),
    )(*arrays)


def moments_kernel(ss, g_ref, m_ref, v_ref, new_m, new_v):
    factor = clip_factor(ss[...])[:1, :1]

    def update(rows):
        g = g_ref[0, 0, rows, :].astype(F32) * factor
        new_m[0, rows, :] = 0.9 * m_ref[0, rows, :] + 0.1 * g
        new_v[0, rows, :] = 0.95 * v_ref[0, rows, :] + 0.05 * g * g

    row_loop(update)


def moments(ss, g, which, m, v):
    own = pl.BlockSpec((1, R, C), (lambda l, q: (l, 0, q)) if which < 2 else (lambda l, q: (l, q, 0)))
    return pl.pallas_call(
        moments_kernel,
        name=f"moments_{which}",
        out_shape=[jax.ShapeDtypeStruct(m.shape, F32)] * 2,
        grid=(LAYERS, Q),
        in_specs=[pl.BlockSpec((8, 128), lambda l, q: (0, 0)), pl.BlockSpec((1, 1, R, C), lambda l, q: (l, which * Q + q, 0, 0)), own, own],
        out_specs=[own, own],
        cost_estimate=COST,
    )(ss, g, m, v)


def move(copies, buf, l_sem, s_sem):
    load = lambda n: pltpu.make_async_copy(copies[n][0], buf.at[n % SLOTS], l_sem.at[n % SLOTS])
    store = lambda n: pltpu.make_async_copy(buf.at[n % SLOTS], copies[n][1], s_sem.at[n % SLOTS])
    total, lag = len(copies), SLOTS // 2
    for t in range(total + lag):
        if t < total:
            if t >= SLOTS:
                store(t - SLOTS).wait()
            load(t).start()
        if t >= lag:
            load(t - lag).wait()
            store(t - lag).start()
    for n in range(max(0, total - SLOTS), total):
        store(n).wait()


def fill_kernel(same, across, later_x, later_y, w0, w1, w2, *scratch):
    me, x, y, xy, _ = neighbours()
    flip = 1 - 2 * lax.rem(me, 2)
    whole = (w0, w1, w2)
    copies = []
    for j in range(CHUNKS):
        for layer in range(2):
            for k, d in enumerate((me, x, y, xy)):
                late = j >= KEPT
                if late and k == 3:
                    continue
                src = same.at[k, layer, j]
                if late and (k, layer) == (2, 0):
                    src = later_x.at[j - KEPT]
                if late and (k, layer) == (1, 1):
                    src = later_y.at[j - KEPT]
                copies.append((src, chunk(whole, j, layer, d)))
                copies.append((across.at[k, layer, j], chunk(whole, j, layer, d + flip)))
    move(copies, *scratch)


def finish_kernel(a0, a1, b0, b1, _0, _1, _2, w0, w1, w2, *scratch):
    me, x, y, xy, _ = neighbours()
    flip = 1 - 2 * lax.rem(me, 2)
    whole = (w0, w1, w2)
    copies = []
    for j in range(KEPT, CHUNKS):
        for layer, a, b in ((0, a0, b0), (1, a1, b1)):
            copies.append((a.at[j - KEPT], chunk(whole, j, layer, xy)))
            copies.append((b.at[j - KEPT], chunk(whole, j, layer, xy + flip)))
    move(copies, *scratch)


def local_call(kernel, name, inputs, like, aliases):
    any_ = pl.BlockSpec(memory_space=pl.ANY)
    return pl.pallas_call(
        kernel,
        name=name,
        out_shape=[jax.ShapeDtypeStruct(w.shape, BF16) for w in like],
        in_specs=[any_] * len(inputs),
        out_specs=[any_] * 3,
        input_output_aliases=aliases,
        scratch_shapes=[pltpu.VMEM((SLOTS, R, C), BF16), pltpu.SemaphoreType.DMA((SLOTS,)), pltpu.SemaphoreType.DMA((SLOTS,))],
        cost_estimate=COST,
    )(*inputs)


def swap_with(array, distance):
    pairs = [(i, i ^ distance) for i in range(8)]
    return lax.ppermute(array, "dp", pairs)


def solution(mesh):
    def step(*arrays):
        terms, weights, m, v = (arrays[i : i + 3] for i in (0, 3, 6, 9))
        g, squares, _, same, across, later_x, later_y = step_call(*arrays)
        a0, a1 = swap_with(later_x, 4), swap_with(later_y, 2)
        whole = local_call(fill_kernel, "fill", (same, across, later_x, later_y), weights, {})
        states = [moments(squares, g, 0, m[0], v[0])]
        a0, a1, g, whole, states = lax.optimization_barrier((a0, a1, g, whole, states))
        b0, b1 = swap_with(a0, 1), swap_with(a1, 1)
        states += [moments(squares, g, i, m[i], v[i]) for i in (1, 2)]
        b0, b1, whole, states = lax.optimization_barrier((b0, b1, whole, states))
        whole = local_call(finish_kernel, "finish", (a0, a1, b0, b1, *whole), weights, {4: 0, 5: 1, 6: 2})
        return (*whole, *(one[0] for one in states), *(one[1] for one in states))

    all_of, cut = P(None, None, None), P(None, "dp", None)
    return jax.shard_map(
        step,
        mesh=mesh,
        in_specs=(P(("rep", "dp"), None, None, None),) * 3 + (all_of,) * 3 + (cut,) * 6,
        out_specs=(P("rep", None, None),) * 3 + (P("rep", "dp", None),) * 6,
        check_vma=False,
    )
```
